512 devices in a mesh: space: 128 (over y, z, core), level: 4 (over x).
Axes of the slice: x: 4, y: 4, z: 16, core: 2. Of those that a mesh axis runs over, the one named last changes fastest.
Arguments:
- grid_latent: bfloat16 [65536, 512], P('space'), may hold values from -6 to 6
- mesh_latent: bfloat16 [4, 1024, 512], P('level', 'space'), may hold values from -6 to 6
- grid_output_cotangent: bfloat16 [65536, 512], P('space'), may hold values from -6 to 6
- w_send: bfloat16 [512, 512], replicated, may hold values from -0.25 to 0.25
- w_recv: bfloat16 [512, 512], replicated, may hold values from -0.25 to 0.25
- output_weight: bfloat16 [512, 512], replicated, may hold values from -0.25 to 0.25
- hidden_layer_bias: float32 [512], replicated, may hold values from -4 to 4
- output_norm_gain: float32 [512], replicated, may hold values from 0.1 to 1.9
- edge_sender: int32 [4, 262144], P('level', 'space'), may hold values from 0 to 23
- edge_receiver: int32 [4, 262144], P('level', 'space'), may hold values from 0 to 511
- edge_live: int32 [4, 262144], P('level', 'space'), may hold values 0 or 1
Outputs:
- d_grid: float32 [65536, 512], P(('space', 'level'))
- d_mesh: float32 [4, 1024, 512], P('level', 'space')
- d_w_send: bfloat16 [512, 512], replicated
- d_w_recv: bfloat16 [512, 512], replicated
- d_w_out: bfloat16 [512, 512], replicated
- d_bias: float32 [512], replicated
- d_gain: float32 [512], replicated
The draws below stay inside these ranges and needn't reach their ends.
All inputs are finite; a program needn't handle non-finite values. No bound on the sum of `edge_live` on one device may be relied on, other than what follows from the above.
Results may differ from the reference program's by a relative error of at most 0.012.
Values may be sent and summed in bfloat16 or wider, within the bound.
A program may use at most 64 MiB of HBM per device.

```python
import jax
import jax.numpy as jnp
from jax import lax

D = 512
G_DEV = 512
MESH_DEV = 8
LEVELS = 4
EDGE_SLOTS_SHARD = 2048
GRID = 65536
MESH_ROWS = 1024
EDGES = 262144
N_SPACE = 128


def plant(result, stream_key, low, high):
    longest = result.shape.index(max(result.shape))
    spots = []
    for shift in (0, 1):
        where = [jax.random.randint(jax.random.fold_in(stream_key, axis), (), 0, length) for axis, length in enumerate(result.shape)]
        where[longest] = (where[longest] + shift) % result.shape[longest]
        spots.append(tuple(where))
    return result.at[spots[0]].set(low).at[spots[1]].set(high)


def block_levels(own_key, extent, pieces, least, top_value):
    def one(dim, blocks):
        heights = jax.random.uniform(jax.random.fold_in(jax.random.fold_in(own_key, 6), dim), (blocks,), jnp.float32, least / len(pieces), top_value / len(pieces))
        return jnp.repeat(jnp.exp(heights), extent[dim] // blocks).reshape((-1,) + (1,) * (len(extent) - dim - 1))

    loudness = one(*pieces[0])
    for cut in pieces[1:]:
        loudness = loudness * one(*cut)
    return loudness


def centred(own_key, extent, spread, bound, pieces=(), kind=jnp.bfloat16):
    result = spread * jax.random.normal(own_key, extent, jnp.float32)
    if pieces:
        result = result * block_levels(own_key, extent, pieces, -0.22, 0.18)
    return jnp.clip(result, -bound, bound).astype(kind)


def setup_inputs(seed: int = 0) -> dict:
    streams_of = jax.random.split(jax.random.key(seed), 12)
    return {
        "grid_latent": centred(streams_of[0], (GRID, D), 1.0, 6.0, ((0, 128),)),
        "mesh_latent": centred(streams_of[1], (LEVELS, MESH_ROWS, D), 1.0, 6.0, ((0, 4), (1, 128))),
        "grid_output_cotangent": centred(streams_of[2], (GRID, D), 1.0, 6.0, ((0, 128),)),
        "w_send": centred(streams_of[3], (D, D), D ** -0.5, 0.25),
        "w_recv": centred(streams_of[4], (D, D), D ** -0.5, 0.25),
        "output_weight": centred(streams_of[5], (D, D), D ** -0.5, 0.25),
        "hidden_layer_bias": centred(streams_of[6], (D,), 0.7, 4.0, (), jnp.float32),
        "output_norm_gain": jnp.clip(1.0 + 0.18 * jax.random.normal(streams_of[7], (D,), jnp.float32), 0.1, 1.9),
        "edge_sender": plant(jax.random.randint(streams_of[8], (LEVELS, EDGES), 0, 3 * MESH_DEV), jax.random.fold_in(streams_of[8], 1), 0, (3 * MESH_DEV) - 1).astype(jnp.int32),
        "edge_receiver": plant(jax.random.randint(streams_of[9], (LEVELS, EDGES), 0, G_DEV), jax.random.fold_in(streams_of[9], 1), 0, G_DEV - 1).astype(jnp.int32),
        "edge_live": plant((jax.random.randint(streams_of[10], (LEVELS, EDGES), 0, 4) < 3).astype(jnp.int32), jax.random.fold_in(streams_of[10], 1), 0, 1),
    }


def edge_reverse_step(sending_rows, receiver_rows, cotangent_lines, slot_active_flags, output_weight, hidden_layer_bias, output_norm_gain):
    preact = sending_rows + receiver_rows + hidden_layer_bias
    hidden = jax.nn.silu(preact).astype(jnp.bfloat16)
    outer = jnp.dot(hidden, output_weight, preferred_element_type=jnp.float32)
    center = outer - lax.optimization_barrier(jnp.mean(outer, axis=-1, keepdims=True))
    inv_scale = lax.rsqrt(lax.optimization_barrier(jnp.mean(center * center, axis=-1, keepdims=True)) + 1e-05)
    normed = center * inv_scale
    incoming_gradient = cotangent_lines.astype(jnp.float32) * slot_active_flags[:, None].astype(jnp.float32)
    scaled = incoming_gradient * output_norm_gain
    d_outer = inv_scale * (scaled - lax.optimization_barrier(jnp.mean(scaled, axis=-1, keepdims=True)) - normed * lax.optimization_barrier(jnp.mean(scaled * normed, axis=-1, keepdims=True)))
    d_outer_b = d_outer.astype(jnp.bfloat16)
    w_out_grad = jnp.dot(hidden.T, d_outer_b, preferred_element_type=jnp.float32)
    d_hidden = jnp.dot(d_outer_b, output_weight.T, preferred_element_type=jnp.float32)
    sigmoid = jax.nn.sigmoid(preact)
    preactivation_gradient = d_hidden * sigmoid * (1.0 + preact * (1.0 - sigmoid))
    return (preactivation_gradient, w_out_grad, lax.optimization_barrier(jnp.sum(preactivation_gradient, axis=0)), lax.optimization_barrier(jnp.sum(incoming_gradient * normed, axis=0)))

def reference(grid_latent, mesh_latent, grid_output_cotangent, w_send, w_recv, output_weight, hidden_layer_bias, output_norm_gain, edge_sender, edge_receiver, edge_live):
    proj_send = jnp.einsum('lmd,de->lme', mesh_latent.astype(jnp.float32), w_send.astype(jnp.float32)).astype(jnp.bfloat16)
    projected_receiver = jnp.dot(grid_latent, w_recv, preferred_element_type=jnp.float32)
    mesh_levels = []
    grid_total = jnp.zeros((GRID, D), jnp.float32)
    wout_acc = jnp.zeros((D, D), jnp.float32)
    bias_acc = jnp.zeros((D,), jnp.float32)
    gain_acc = jnp.zeros((D,), jnp.float32)
    for level in range(LEVELS):
        level_table = proj_send[level]
        senders = edge_sender[level]
        receivers = edge_receiver[level]
        active_slots = edge_live[level]

        def visit(carry, shard):
            mesh_acc, grid_acc, wout_sum, bias_sum, gain_sum = carry
            start_offset = (shard * EDGE_SLOTS_SHARD).astype(jnp.int32)
            sender_local = lax.dynamic_slice_in_dim(senders, start_offset, EDGE_SLOTS_SHARD)
            recv_local = lax.dynamic_slice_in_dim(receivers, start_offset, EDGE_SLOTS_SHARD)
            slot_active_flags = lax.dynamic_slice_in_dim(active_slots, start_offset, EDGE_SLOTS_SHARD)
            target = shard + sender_local // MESH_DEV - 1
            target = jnp.where((target < 0) | (target >= N_SPACE), shard, target).astype(jnp.int32)
            global_row = (target * MESH_DEV + sender_local % MESH_DEV).astype(jnp.int32)
            receiver_index = (recv_local + shard * G_DEV).astype(jnp.int32)
            sending_rows = level_table[global_row].astype(jnp.float32)
            preactivation_gradient, output_weight_piece, bias_piece, gain_piece = edge_reverse_step(sending_rows, projected_receiver[receiver_index], grid_output_cotangent[receiver_index], slot_active_flags, output_weight, hidden_layer_bias, output_norm_gain)
            mesh_acc = mesh_acc.at[global_row].add(preactivation_gradient)
            grid_acc = grid_acc.at[receiver_index].add(preactivation_gradient)
            return ((mesh_acc, grid_acc, wout_sum + output_weight_piece, bias_sum + bias_piece, gain_sum + gain_piece), None)
        start_carry = (jnp.zeros((MESH_ROWS, D), jnp.float32), jnp.zeros((GRID, D), jnp.float32), wout_acc, bias_acc, gain_acc)
        final, _ = lax.scan(visit, start_carry, jnp.arange(N_SPACE, dtype=jnp.int32))
        mesh_level, grid_level, wout_acc, bias_acc, gain_acc = final
        mesh_levels.append(mesh_level)
        grid_total = grid_total + grid_level.astype(jnp.bfloat16).astype(jnp.float32)
    mesh_sum = jnp.stack(mesh_levels, axis=0).astype(jnp.bfloat16)
    grid_sum = grid_total.astype(jnp.bfloat16)
    d_mesh = jnp.einsum('lmd,ed->lme', mesh_sum.astype(jnp.float32), w_send.astype(jnp.float32))
    d_grid = jnp.dot(grid_sum, w_recv.T, preferred_element_type=jnp.float32)
    d_w_send = jnp.einsum('lmd,lme->de', mesh_latent.astype(jnp.float32), mesh_sum.astype(jnp.float32))
    d_w_recv = jnp.dot(grid_latent.T, grid_sum, preferred_element_type=jnp.float32)
    return (d_grid, d_mesh, d_w_send.astype(jnp.bfloat16), d_w_recv.astype(jnp.bfloat16), wout_acc.astype(jnp.bfloat16), bias_acc, gain_acc)
```

```python
import jax
import jax.numpy as jnp
from jax import lax
from jax.experimental import pallas as pl
from jax.experimental.pallas import tpu as pltpu
from jax.sharding import PartitionSpec as P

F32 = jnp.float32
BF16 = jnp.bfloat16
NT = (((1,), (1,)), ((), ()))
TN = (((0,), (0,)), ((), ()))
PAD = 128
BLOCK = 256


def mm(a, b, dims=(((1,), (0,)), ((), ()))):
    return lax.dot_general(a, b, dims, preferred_element_type=F32)


def edge_kernel(
    grid_ref,
    cot_ref,
    win_ref,
    w_send_ref,
    w_recv_ref,
    w_out_ref,
    bias_ref,
    gain_ref,
    recv_ref,
    row_ref,
    g_ref,
    vec_ref,
    level_ref,
    table_grad_ref,
    table,
    pick,
    pick_t,
    hid,
    dact,
    douter,
    dpre,
):
    grid_rows, width = grid_ref.shape
    slots = recv_ref.shape[1]
    window = win_ref.shape[0]
    table[0:grid_rows] = mm(grid_ref[...], w_recv_ref[...]).astype(BF16)
    table[grid_rows : grid_rows + PAD] = jnp.zeros((PAD, width), BF16)
    table[grid_rows : grid_rows + window] = mm(win_ref[...], w_send_ref[...]).astype(BF16)

    def build(i, carry):
        at = pl.multiple_of(i * 128, 128)
        recv = recv_ref[:, pl.ds(at, 128)]
        row = row_ref[:, pl.ds(at, 128)]
        recv_b = jnp.broadcast_to(recv, (128, 128))
        row_b = jnp.broadcast_to(row, (128, 128))
        recv_c = recv_b.T
        row_c = row_b.T
        lane = lax.broadcasted_iota(jnp.int32, (128, 128), 1)
        sub = lax.broadcasted_iota(jnp.int32, (128, 128), 0)
        for k in range(grid_rows // 128):
            pick[pl.ds(at, 128), k * 128 : (k + 1) * 128] = (lane + k * 128 == recv_c).astype(
                F32
            ).astype(BF16)
            pick_t[k * 128 : (k + 1) * 128, pl.ds(at, 128)] = (sub + k * 128 == recv_b).astype(
                F32
            ).astype(BF16)
        pick[pl.ds(at, 128), grid_rows : grid_rows + PAD] = (lane == row_c).astype(F32).astype(BF16)
        pick_t[grid_rows : grid_rows + PAD, pl.ds(at, 128)] = (
            (sub == row_b).astype(F32).astype(BF16)
        )
        return carry

    lax.fori_loop(0, slots // 128, build, 0)
    bias = bias_ref[...]
    gain = gain_ref[...]
    scale = 1.0 / width

    def forward(i, acc):
        at = pl.multiple_of(i * BLOCK, BLOCK)
        rows = pl.ds(at, BLOCK)
        preact = mm(pick[rows, :], table[...]) + bias
        sig = jax.nn.sigmoid(preact)
        hidden = preact * sig
        hidden_b = hidden.astype(BF16)
        hid[rows, :] = hidden_b
        dact[rows, :] = sig + hidden * (1.0 - sig)
        outer = mm(hidden_b, w_out_ref[...])
        upstream = mm(pick[rows, 0:grid_rows], cot_ref[...])
        center = outer - jnp.sum(outer, axis=-1, keepdims=True) * scale
        inv = lax.rsqrt(jnp.sum(center * center, axis=-1, keepdims=True) * scale + 1e-05)
        normed = center * inv
        scaled = upstream * gain
        m1 = jnp.sum(scaled, axis=-1, keepdims=True) * scale
        m2 = jnp.sum(scaled * normed, axis=-1, keepdims=True) * scale
        douter[rows, :] = (inv * (scaled - m1 - normed * m2)).astype(BF16)
        part = upstream * normed
        return acc + jnp.sum(part.reshape(BLOCK // 8, 8, width), axis=0)

    gain_acc = lax.fori_loop(0, slots // BLOCK, forward, jnp.zeros((8, width), F32))
    g_ref[2 * width : 3 * width] = mm(hid[...], douter[...], TN).astype(g_ref.dtype)

    def backward(i, acc):
        at = pl.multiple_of(i * BLOCK, BLOCK)
        rows = pl.ds(at, BLOCK)
        d_pre = mm(douter[rows, :], w_out_ref[...], NT) * dact[rows, :]
        dpre[rows, :] = d_pre.astype(BF16)
        return acc + jnp.sum(d_pre.reshape(BLOCK // 8, 8, width), axis=0)

    bias_acc = lax.fori_loop(0, slots // BLOCK, backward, jnp.zeros((8, width), F32))
    vec_ref[0:1] = jnp.sum(bias_acc, axis=0, keepdims=True)
    vec_ref[1:2] = jnp.sum(gain_acc, axis=0, keepdims=True)
    sums = mm(pick_t[...], dpre[...])
    level = sums[0:grid_rows].astype(BF16)
    level_ref[...] = level
    grads = sums[grid_rows : grid_rows + window]
    table_grad_ref[...] = grads
    g_ref[width : 2 * width] = mm(grid_ref[...], level, TN).astype(g_ref.dtype)
    g_ref[0:width] = mm(win_ref[...], grads.astype(BF16), TN).astype(g_ref.dtype)


def edge_call(grid, cot, win, w_send, w_recv, w_out, bias, gain, recv, row, g_dtype=F32):
    grid_rows, width = grid.shape
    slots = recv.shape[1]
    vmem = pl.BlockSpec(memory_space=pltpu.VMEM)
    flops = 2 * slots * width * width * 7
    return pl.pallas_call(
        edge_kernel,
        out_shape=(
            jax.ShapeDtypeStruct((3 * width, width), g_dtype),
            jax.ShapeDtypeStruct((2, width), F32),
            jax.ShapeDtypeStruct((grid_rows, width), BF16),
            jax.ShapeDtypeStruct((win.shape[0], width), F32),
        ),
        in_specs=[vmem] * 10,
        out_specs=(vmem,) * 4,
        scratch_shapes=[
            pltpu.VMEM((grid_rows + PAD, width), BF16),
            pltpu.VMEM((slots, grid_rows + PAD), BF16),
            pltpu.VMEM((grid_rows + PAD, slots), BF16),
            pltpu.VMEM((slots, width), BF16),
            pltpu.VMEM((slots, width), F32),
            pltpu.VMEM((slots, width), BF16),
            pltpu.VMEM((slots, width), BF16),
        ],
        compiler_params=pltpu.CompilerParams(vmem_limit_bytes=48 * 1024 * 1024),
        cost_estimate=pl.CostEstimate(flops=flops, bytes_accessed=8 << 20, transcendentals=0),
    )(grid, cot, win, w_send, w_recv, w_out, bias, gain, recv, row)


def rows_of(edge_sender, edge_receiver, edge_live, mesh_rows):
    sender = edge_sender[0:1]
    band = lax.axis_index("space")
    target = band + sender // mesh_rows - 1
    inside = (target >= 0) & (target < lax.axis_size("space"))
    row = jnp.where(inside, sender, mesh_rows + sender % mesh_rows)
    recv = jnp.where(edge_live[0:1] > 0, edge_receiver[0:1], -1)
    return recv, row


def from_behind(block, axis, distance):
    devices = range(lax.axis_size(axis))
    route = [(i - distance, i) for i in devices if i - distance in devices]
    return lax.ppermute(block, axis, route)


def body(
    grid_latent,
    mesh_latent,
    grid_output_cotangent,
    w_send,
    w_recv,
    output_weight,
    hidden_layer_bias,
    output_norm_gain,
    edge_sender,
    edge_receiver,
    edge_live,
):
    width = grid_latent.shape[1]
    grid_rows = grid_latent.shape[0]
    mesh_rows = mesh_latent.shape[1]
    own = mesh_latent[0]
    win = jnp.concatenate(
        [
            from_behind(own, "space", 1),
            own,
            from_behind(own, "space", -1),
            jnp.zeros((mesh_rows, width), BF16),
        ],
        axis=0,
    )
    recv, row = rows_of(edge_sender, edge_receiver, edge_live, mesh_rows)
    g, vec, level, grads = edge_call(
        grid_latent,
        grid_output_cotangent,
        win,
        w_send,
        w_recv,
        output_weight,
        hidden_layer_bias[None],
        output_norm_gain[None],
        recv,
        row,
        BF16,
    )
    below = grads[:mesh_rows]
    above = grads[2 * mesh_rows : 3 * mesh_rows]
    mesh_acc = (
        grads[mesh_rows : 2 * mesh_rows]
        + from_behind(above, "space", 1)
        + from_behind(below, "space", -1)
    )
    levels = lax.axis_size("level")
    tiles = lax.all_to_all(level.reshape(levels, -1, width), "level", 0, 0, tiled=True)
    grid_sum = jnp.sum(tiles.astype(F32), axis=0).astype(BF16)
    d_mesh = jnp.dot(mesh_acc.astype(BF16), w_send.T, preferred_element_type=F32)[None]
    d_grid = jnp.dot(grid_sum, w_recv.T, preferred_element_type=F32)
    total, vec = lax.psum((g.astype(F32), vec), ("space", "level"))
    total = total.astype(BF16)
    return (
        d_grid,
        d_mesh,
        total[:width],
        total[width : 2 * width],
        total[2 * width :],
        vec[0],
        vec[1],
    )


def solution(mesh):
    return jax.shard_map(
        body,
        mesh=mesh,
        in_specs=(
            P("space", None),
            P("level", "space", None),
            P("space", None),
            P(),
            P(),
            P(),
            P(),
            P(),
            P("level", "space"),
            P("level", "space"),
            P("level", "space"),
        ),
        out_specs=(P(("space", "level"), None), P("level", "space", None), P(), P(), P(), P(), P()),
        check_vma=False,
    )
```

```python
import jax
import jax.numpy as jnp
from jax import lax
from jax.experimental import pallas as pl
from jax.experimental.pallas import tpu as pltpu
from jax.sharding import PartitionSpec as P

F32 = jnp.float32
BF16 = jnp.bfloat16
NT = (((1,), (1,)), ((), ()))
TN = (((0,), (0,)), ((), ()))
PAD = 128
BLOCK = 256


def mm(a, b, dims=(((1,), (0,)), ((), ()))):
    return lax.dot_general(a, b, dims, preferred_element_type=F32)


def edge_kernel(
    grid_ref,
    cot_ref,
    win_ref,
    w_send_ref,
    w_recv_ref,
    w_out_ref,
    bias_ref,
    gain_ref,
    recv_ref,
    row_ref,
    g_ref,
    vec_ref,
    level_ref,
    table_grad_ref,
    table,
    pick,
    pick_t,
    hid,
    dact,
    douter,
    dpre,
):
    grid_rows, width = grid_ref.shape
    slots = recv_ref.shape[1]
    window = win_ref.shape[0]
    table[0:grid_rows] = mm(grid_ref[...], w_recv_ref[...]).astype(BF16)
    table[grid_rows : grid_rows + PAD] = jnp.zeros((PAD, width), BF16)
    table[grid_rows : grid_rows + window] = mm(win_ref[...], w_send_ref[...]).astype(BF16)

    def build(i, carry):
        at = pl.multiple_of(i * 128, 128)
        recv = recv_ref[:, pl.ds(at, 128)]
        row = row_ref[:, pl.ds(at, 128)]
        recv_b = jnp.broadcast_to(recv, (128, 128))
        row_b = jnp.broadcast_to(row, (128, 128))
        recv_c = recv_b.T
        row_c = row_b.T
        lane = lax.broadcasted_iota(jnp.int32, (128, 128), 1)
        sub = lax.broadcasted_iota(jnp.int32, (128, 128), 0)
        for k in range(grid_rows // 128):
            pick[pl.ds(at, 128), k * 128 : (k + 1) * 128] = (lane + k * 128 == recv_c).astype(
                F32
            ).astype(BF16)
            pick_t[k * 128 : (k + 1) * 128, pl.ds(at, 128)] = (sub + k * 128 == recv_b).astype(
                F32
            ).astype(BF16)
        pick[pl.ds(at, 128), grid_rows : grid_rows + PAD] = (lane == row_c).astype(F32).astype(BF16)
        pick_t[grid_rows : grid_rows + PAD, pl.ds(at, 128)] = (
            (sub == row_b).astype(F32).astype(BF16)
        )
        return carry

    lax.fori_loop(0, slots // 128, build, 0)
    bias = bias_ref[...]
    gain = gain_ref[...]
    scale = 1.0 / width

    def forward(i, acc):
        at = pl.multiple_of(i * BLOCK, BLOCK)
        rows = pl.ds(at, BLOCK)
        preact = mm(pick[rows, :], table[...]) + bias
        sig = jax.nn.sigmoid(preact)
        hidden = preact * sig
        hidden_b = hidden.astype(BF16)
        hid[rows, :] = hidden_b
        dact[rows, :] = sig + hidden * (1.0 - sig)
        outer = mm(hidden_b, w_out_ref[...])
        upstream = mm(pick[rows, 0:grid_rows], cot_ref[...])
        center = outer - jnp.sum(outer, axis=-1, keepdims=True) * scale
        inv = lax.rsqrt(jnp.sum(center * center, axis=-1, keepdims=True) * scale + 1e-05)
        normed = center * inv
        scaled = upstream * gain
        m1 = jnp.sum(scaled, axis=-1, keepdims=True) * scale
        m2 = jnp.sum(scaled * normed, axis=-1, keepdims=True) * scale
        douter[rows, :] = (inv * (scaled - m1 - normed * m2)).astype(BF16)
        part = upstream * normed
        return acc + jnp.sum(part.reshape(BLOCK // 8, 8, width), axis=0)

    gain_acc = lax.fori_loop(0, slots // BLOCK, forward, jnp.zeros((8, width), F32))
    g_ref[2 * width : 3 * width] = mm(hid[...], douter[...], TN).astype(g_ref.dtype)

    def backward(i, acc):
        at = pl.multiple_of(i * BLOCK, BLOCK)
        rows = pl.ds(at, BLOCK)
        d_pre = mm(douter[rows, :], w_out_ref[...], NT) * dact[rows, :]
        dpre[rows, :] = d_pre.astype(BF16)
        return acc + jnp.sum(d_pre.reshape(BLOCK // 8, 8, width), axis=0)

    bias_acc = lax.fori_loop(0, slots // BLOCK, backward, jnp.zeros((8, width), F32))
    vec_ref[0:1] = jnp.sum(bias_acc, axis=0, keepdims=True)
    vec_ref[1:2] = jnp.sum(gain_acc, axis=0, keepdims=True)
    sums = mm(pick_t[...], dpre[...])
    level = sums[0:grid_rows].astype(BF16)
    level_ref[...] = level
    grads = sums[grid_rows : grid_rows + window]
    table_grad_ref[...] = grads
    g_ref[width : 2 * width] = mm(grid_ref[...], level, TN).astype(g_ref.dtype)
    g_ref[0:width] = mm(win_ref[...], grads.astype(BF16), TN).astype(g_ref.dtype)


def edge_call(grid, cot, win, w_send, w_recv, w_out, bias, gain, recv, row, g_dtype=F32):
    grid_rows, width = grid.shape
    slots = recv.shape[1]
    vmem = pl.BlockSpec(memory_space=pltpu.VMEM)
    flops = 2 * slots * width * width * 7
    return pl.pallas_call(
        edge_kernel,
        out_shape=(
            jax.ShapeDtypeStruct((3 * width, width), g_dtype),
            jax.ShapeDtypeStruct((2, width), F32),
            jax.ShapeDtypeStruct((grid_rows, width), BF16),
            jax.ShapeDtypeStruct((win.shape[0], width), F32),
        ),
        in_specs=[vmem] * 10,
        out_specs=(vmem,) * 4,
        scratch_shapes=[
            pltpu.VMEM((grid_rows + PAD, width), BF16),
            pltpu.VMEM((slots, grid_rows + PAD), BF16),
            pltpu.VMEM((grid_rows + PAD, slots), BF16),
            pltpu.VMEM((slots, width), BF16),
            pltpu.VMEM((slots, width), F32),
            pltpu.VMEM((slots, width), BF16),
            pltpu.VMEM((slots, width), BF16),
        ],
        compiler_params=pltpu.CompilerParams(vmem_limit_bytes=48 * 1024 * 1024),
        cost_estimate=pl.CostEstimate(flops=flops, bytes_accessed=8 << 20, transcendentals=0),
    )(grid, cot, win, w_send, w_recv, w_out, bias, gain, recv, row)


MESH = pl.DeviceIdType.MESH
DEPTH = 16
NEAR = 4
CHUNKS = ((2, "yx"), (1, "xy"), (0, "yx"))


class Ring:
    def __init__(self):
        space = lax.axis_index("space")
        self.count = lax.axis_size("space")
        self.x = lax.axis_index("level")
        self.nx = lax.axis_size("level")
        self.ny = self.count // (2 * DEPTH)
        self.space = space
        self.core = lax.rem(space, 2)
        z = lax.rem(space // 2, DEPTH)
        self.y = space // (2 * DEPTH)
        self.near = lax.rem(z, NEAR)
        self.far = z // NEAR

    def at(self, core=None, y=None, near=None, far=None, x=None):
        core = self.core if core is None else core
        y = self.y if y is None else y
        near = self.near if near is None else near
        far = self.far if far is None else far
        x = self.x if x is None else x
        return {"space": ((y * DEPTH) + far * NEAR + near) * 2 + core, "level": x}

    def peers(self, axis):
        me, n = {
            "core": (self.core, 2),
            "y": (self.y, self.ny),
            "x": (self.x, self.nx),
            "near": (self.near, NEAR),
            "far": (self.far, DEPTH // NEAR),
        }[axis]
        out = []
        for d in range(1, n):
            to = lax.rem(me + d, n)
            out.append((d, to, self.at(**{axis: to})))
        return me, n, out

    def beside(self, step):
        return {"space": lax.rem(self.space + step + self.count, self.count), "level": self.x}


class Copies:
    def __init__(self, send_sem, recv_sem):
        self.send_sem, self.recv_sem = send_sem, recv_sem
        self.used = 0
        self.all = []

    def start(self, src, dst, device):
        k = self.used
        self.used += 1
        copy = pltpu.make_async_remote_copy(
            src_ref=src,
            dst_ref=dst,
            send_sem=self.send_sem.at[k],
            recv_sem=self.recv_sem.at[k],
            device_id=device,
            device_id_type=MESH,
        )
        copy.start()
        self.all.append(copy)
        return copy

    def finish(self):
        for copy in self.all:
            copy.wait_send()


def span(start, size, step):
    return pl.ds(pl.multiple_of(start, step), size)


class Reduce:
    def __init__(self, ring, copies, index, order, g_ref, out_ref, bufs):
        self.ring, self.copies = ring, copies
        self.order = order
        self.g, self.out = g_ref, out_ref
        self.core_buf, self.acc1, self.buf1, self.acc2, self.buf2, self.acc3, self.buf3, self.buf4 = bufs
        self.width = g_ref.shape[1]
        rows = self.width
        self.rows = rows
        self.n1 = rows // 2
        self.n2 = self.n1 // 4
        self.n3 = self.n2 // 4
        self.base = index * rows
        self.b1, self.b2, self.b3 = index * self.n1, index * self.n2, index * self.n3
        self.cols = self.width // NEAR

    def wait(self):
        for copy in self.flight:
            copy.wait_recv()

    def mine(self, level, a1=None, a2=None):
        r = self.ring
        at = self.base + r.core * self.n1
        if level >= 1:
            at = at + (getattr(r, self.order[0]) if a1 is None else a1) * self.n2
        if level >= 2:
            at = at + (getattr(r, self.order[1]) if a2 is None else a2) * self.n3
        return span(at, (self.n1, self.n2, self.n3)[level], 16)

    def s0(self):
        r = self.ring
        _, _, peers = r.peers("core")
        ((_, other, device),) = peers
        src = self.g.at[span(self.base + other * self.n1, self.n1, 16)]
        self.flight = [self.copies.start(src, self.core_buf.at[pl.ds(self.b1, self.n1)], device)]

    def s1(self):
        self.wait()
        mine = self.g[self.mine(0), :].astype(F32)
        here = pl.ds(self.b1, self.n1)
        self.acc1[here] = (mine + self.core_buf[here].astype(F32)).astype(BF16)
        _, _, peers = self.ring.peers(self.order[0])
        self.flight = []
        for d, to, device in peers:
            src = self.acc1.at[span(self.b1 + to * self.n2, self.n2, 16)]
            dst = self.buf1.at[d - 1, pl.ds(self.b2, self.n2)]
            self.flight.append(self.copies.start(src, dst, device))

    def s2(self):
        self.wait()
        me, n, _ = self.ring.peers(self.order[0])
        total = self.acc1[span(self.b1 + me * self.n2, self.n2, 16), :].astype(F32)
        here = pl.ds(self.b2, self.n2)
        for d in range(n - 1):
            total = total + self.buf1[d, here].astype(F32)
        self.acc2[here] = total.astype(BF16)
        _, _, peers = self.ring.peers(self.order[1])
        self.flight = []
        for d, to, device in peers:
            src = self.acc2.at[span(self.b2 + to * self.n3, self.n3, 16)]
            dst = self.buf2.at[d - 1, pl.ds(self.b3, self.n3)]
            self.flight.append(self.copies.start(src, dst, device))

    def s3(self):
        self.wait()
        me, n, _ = self.ring.peers(self.order[1])
        total = self.acc2[span(self.b2 + me * self.n3, self.n3, 16), :].astype(F32)
        here = pl.ds(self.b3, self.n3)
        for d in range(n - 1):
            total = total + self.buf2[d, here].astype(F32)
        self.acc3[here] = total.astype(BF16)
        _, _, peers = self.ring.peers("near")
        self.flight = []
        for d, to, device in peers:
            src = self.acc3.at[here, span(to * self.cols, self.cols, 128)]
            dst = self.buf3.at[d - 1, here]
            self.flight.append(self.copies.start(src, dst, device))

    def s4(self):
        self.wait()
        me, n, _ = self.ring.peers("near")
        here = pl.ds(self.b3, self.n3)
        total = self.acc3[here, span(me * self.cols, self.cols, 128)].astype(F32)
        for d in range(n - 1):
            total = total + self.buf3[d, here].astype(F32)
        far, _, peers = self.ring.peers("far")
        self.buf4[far, here] = total.astype(BF16)
        self.flight = []
        for _, _, device in peers:
            slot = self.buf4.at[far, here]
            self.flight.append(self.copies.start(slot, slot, device))

    def s5(self):
        self.wait()
        here = pl.ds(self.b3, self.n3)
        _, n, _ = self.ring.peers("far")
        total = self.buf4[0, here].astype(F32)
        for k in range(1, n):
            total = total + self.buf4[k, here].astype(F32)
        me, _, peers = self.ring.peers("near")
        rows, cols = self.mine(2), span(me * self.cols, self.cols, 128)
        self.out[rows, cols] = total.astype(BF16)
        self.flight = []
        for _, _, device in peers:
            part = self.out.at[rows, cols]
            self.flight.append(self.copies.start(part, part, device))

    def spread(self, axis, level):
        self.wait()
        _, _, peers = self.ring.peers(axis)
        part = self.out.at[self.mine(level)]
        self.flight = [self.copies.start(part, part, device) for _, _, device in peers]

    def s6(self):
        self.spread(self.order[1], 2)

    def s7(self):
        self.spread(self.order[0], 1)

    def s8(self):
        self.spread("core", 0)

    def s9(self):
        self.wait()


class Vector:
    AXES = ("core", "y", "x", "near", "far")

    def __init__(self, ring, copies, buf):
        self.ring, self.copies, self.buf = ring, copies, buf
        self.step = 0

    def start(self, value):
        me, n, peers = self.ring.peers(self.AXES[self.step])
        self.buf[self.step, me] = value
        slot = self.buf.at[self.step, me]
        self.flight = [self.copies.start(slot, slot, device) for _, _, device in peers]
        self.n = n

    def total(self):
        for copy in self.flight:
            copy.wait_recv()
        total = self.buf[self.step, 0]
        for k in range(1, self.n):
            total = total + self.buf[self.step, k]
        self.step += 1
        return total

    def next(self):
        self.start(self.total())


def greet(ring):
    barrier = pltpu.get_barrier_semaphore()
    count = 0
    for axis in ("far", "near", "y", "x", "core"):
        for _, _, device in ring.peers(axis)[2]:
            pl.semaphore_signal(barrier, inc=1, device_id=device, device_id_type=MESH)
            count += 1
    outer = ring.beside(2 * ring.core - 1)
    pl.semaphore_signal(barrier, inc=1, device_id=outer, device_id_type=MESH)
    return barrier, count + 1


def comm_kernel(
    g_ref,
    vec_ref,
    level_ref,
    grads_ref,
    w_send_ref,
    w_recv_ref,
    out_ref,
    vec_out_ref,
    d_grid_ref,
    d_mesh_ref,
    out,
    core_buf,
    acc1,
    buf1,
    acc2,
    buf2,
    acc3,
    buf3,
    buf4,
    vec_buf,
    level_buf,
    halo_buf,
    send_sem,
    recv_sem,
):
    ring = Ring()
    barrier, count = greet(ring)
    pl.semaphore_wait(barrier, count)
    copies = Copies(send_sem, recv_sem)
    bufs = (core_buf, acc1, buf1, acc2, buf2, acc3, buf3, buf4)
    parts = [Reduce(ring, copies, i, order, g_ref, out, bufs) for i, order in CHUNKS]
    vec = Vector(ring, copies, vec_buf)
    for part in parts:
        part.s0()
    vec.start(vec_ref[...])
    for part in parts:
        part.s1()
    vec.next()
    mesh_rows = halo_buf.shape[1]
    halo = [
        copies.start(grads_ref.at[pl.ds(2 * mesh_rows, mesh_rows)], halo_buf.at[0], ring.beside(1)),
        copies.start(grads_ref.at[pl.ds(0, mesh_rows)], halo_buf.at[1], ring.beside(-1)),
    ]
    for part in parts:
        part.s2()
    vec.next()
    share = level_buf.shape[1]
    x, _, x_peers = ring.peers("x")
    levels = []
    for d, to, device in x_peers:
        src = level_ref.at[span(to * share, share, 16)]
        levels.append(copies.start(src, level_buf.at[d - 1], device))
    for part in parts:
        part.s3()
    vec.next()
    for part in parts:
        part.s4()
    vec.next()
    for copy in halo:
        copy.wait_recv()
    mesh_sum = grads_ref[mesh_rows : 2 * mesh_rows] + halo_buf[0] + halo_buf[1]
    d_mesh_ref[...] = mm(mesh_sum.astype(BF16), w_send_ref[...], NT)
    for copy in levels:
        copy.wait_recv()
    grid_sum = level_ref[span(x * share, share, 16), :].astype(F32)
    for d in range(len(levels)):
        grid_sum = grid_sum + level_buf[d].astype(F32)
    d_grid_ref[...] = mm(grid_sum.astype(BF16), w_recv_ref[...], NT)
    for part in parts:
        part.s5()
    vec_out_ref[...] = vec.total()
    for part in parts:
        part.s6()
    for part in parts:
        part.s7()
    for part in parts:
        part.s8()
    for part in parts:
        part.s9()
    out_ref[...] = out[...]
    copies.finish()


def comm_scratch(width, grid_rows, mesh_rows, nx, ny):
    rows = 3 * width
    n1 = rows // 2
    n2 = n1 // 4
    n3 = n2 // 4
    cols = width // NEAR
    far = DEPTH // NEAR
    copies = 3 * (1 + 1 + 4 * (nx - 1 + ny - 1)) + 3 * 3 * (NEAR - 1) + 3 * (far - 1)
    copies = 160
    return [
        pltpu.VMEM((rows, width), BF16),
        pltpu.VMEM((n1, width), BF16),
        pltpu.VMEM((n1, width), BF16),
        pltpu.VMEM((3, n2, width), BF16),
        pltpu.VMEM((n2, width), BF16),
        pltpu.VMEM((3, n3, width), BF16),
        pltpu.VMEM((n3, width), BF16),
        pltpu.VMEM((NEAR - 1, n3, cols), BF16),
        pltpu.VMEM((far, n3, cols), BF16),
        pltpu.VMEM((5, 4, 8, 2 * width // 8), F32),
        pltpu.VMEM((nx - 1, grid_rows // nx, width), BF16),
        pltpu.VMEM((2, mesh_rows, width), F32),
        pltpu.SemaphoreType.DMA((copies,)),
        pltpu.SemaphoreType.DMA((copies,)),
    ]


def comm_call(g, vec, level, grads, w_send, w_recv, mesh_rows):
    width = g.shape[1]
    grid_rows = level.shape[0]
    nx = lax.axis_size("level")
    ny = lax.axis_size("space") // (2 * DEPTH)
    vmem = pl.BlockSpec(memory_space=pltpu.VMEM)
    return pl.pallas_call(
        comm_kernel,
        out_shape=(
            jax.ShapeDtypeStruct(g.shape, BF16),
            jax.ShapeDtypeStruct(vec.shape, F32),
            jax.ShapeDtypeStruct((grid_rows // nx, width), F32),
            jax.ShapeDtypeStruct((mesh_rows, width), F32),
        ),
        in_specs=[vmem] * 6,
        out_specs=(vmem,) * 4,
        scratch_shapes=comm_scratch(width, grid_rows, mesh_rows, nx, ny),
        compiler_params=pltpu.CompilerParams(
            vmem_limit_bytes=32 * 1024 * 1024, collective_id=0, has_side_effects=True
        ),
    )(g, vec, level, grads, w_send, w_recv)


def rows_of(edge_sender, edge_receiver, edge_live, mesh_rows):
    sender = edge_sender[0:1]
    band = lax.axis_index("space")
    target = band + sender // mesh_rows - 1
    inside = (target >= 0) & (target < lax.axis_size("space"))
    row = jnp.where(inside, sender, mesh_rows + sender % mesh_rows)
    recv = jnp.where(edge_live[0:1] > 0, edge_receiver[0:1], -1)
    return recv, row


def from_behind(block, axis, distance):
    devices = range(lax.axis_size(axis))
    route = [(i - distance, i) for i in devices if i - distance in devices]
    return lax.ppermute(block, axis, route)


def body(
    grid_latent,
    mesh_latent,
    grid_output_cotangent,
    w_send,
    w_recv,
    output_weight,
    hidden_layer_bias,
    output_norm_gain,
    edge_sender,
    edge_receiver,
    edge_live,
):
    width = grid_latent.shape[1]
    grid_rows = grid_latent.shape[0]
    mesh_rows = mesh_latent.shape[1]
    own = mesh_latent[0]
    win = jnp.concatenate(
        [
            from_behind(own, "space", 1),
            own,
            from_behind(own, "space", -1),
            jnp.zeros((mesh_rows, width), BF16),
        ],
        axis=0,
    )
    recv, row = rows_of(edge_sender, edge_receiver, edge_live, mesh_rows)
    g, vec, level, grads = edge_call(
        grid_latent,
        grid_output_cotangent,
        win,
        w_send,
        w_recv,
        output_weight,
        hidden_layer_bias[None],
        output_norm_gain[None],
        recv,
        row,
        BF16,
    )
    total, vec, d_grid, d_mesh = comm_call(
        g, vec.reshape(8, 2 * width // 8), level, grads, w_send, w_recv, mesh_rows
    )
    vec = vec.reshape(2, width)
    return (
        d_grid,
        d_mesh[None],
        total[:width],
        total[width : 2 * width],
        total[2 * width :],
        vec[0],
        vec[1],
    )


def solution(mesh):
    return jax.shard_map(
        body,
        mesh=mesh,
        in_specs=(
            P("space", None),
            P("level", "space", None),
            P("space", None),
            P(),
            P(),
            P(),
            P(),
            P(),
            P("level", "space"),
            P("level", "space"),
            P("level", "space"),
        ),
        out_specs=(P(("space", "level"), None), P("level", "space", None), P(), P(), P(), P(), P()),
        check_vma=False,
    )
```

```python
import jax
import jax.numpy as jnp
from jax import lax
from jax.experimental import pallas as pl
from jax.experimental.pallas import tpu as pltpu
from jax.sharding import PartitionSpec as P

F32 = jnp.float32
BF16 = jnp.bfloat16
NT = (((1,), (1,)), ((), ()))
TN = (((0,), (0,)), ((), ()))
PAD = 128
BLOCK = 256
PREP_VMEM = 24 << 20
MAIN_VMEM = 40 << 20


def mm(a, b, dims=(((1,), (0,)), ((), ()))):
    return lax.dot_general(a, b, dims, preferred_element_type=F32)


MESH = pl.DeviceIdType.MESH
DEPTH = 16
NEAR = 4
EARLY = ((2, "yx"),)
LATE = ((1, "xy"), (0, "yx"))


class Ring:
    def __init__(self):
        space = lax.axis_index("space")
        self.count = lax.axis_size("space")
        self.x = lax.axis_index("level")
        self.nx = lax.axis_size("level")
        self.ny = self.count // (2 * DEPTH)
        self.space = space
        self.core = lax.rem(space, 2)
        z = lax.rem(space // 2, DEPTH)
        self.y = space // (2 * DEPTH)
        self.near = lax.rem(z, NEAR)
        self.far = z // NEAR

    def at(self, core=None, y=None, near=None, far=None, x=None):
        core = self.core if core is None else core
        y = self.y if y is None else y
        near = self.near if near is None else near
        far = self.far if far is None else far
        x = self.x if x is None else x
        return {"space": ((y * DEPTH) + far * NEAR + near) * 2 + core, "level": x}

    def peers(self, axis):
        me, n = {
            "core": (self.core, 2),
            "y": (self.y, self.ny),
            "x": (self.x, self.nx),
            "near": (self.near, NEAR),
            "far": (self.far, DEPTH // NEAR),
        }[axis]
        out = []
        for d in range(1, n):
            to = lax.rem(me + d, n)
            out.append((d, to, self.at(**{axis: to})))
        return me, n, out

    def beside(self, step):
        return {"space": lax.rem(self.space + step + self.count, self.count), "level": self.x}


class Copies:
    def __init__(self, send_sem, recv_sem):
        self.send_sem, self.recv_sem = send_sem, recv_sem
        self.used = 0
        self.all = []

    def start(self, src, dst, device):
        k = self.used
        self.used += 1
        copy = pltpu.make_async_remote_copy(
            src_ref=src,
            dst_ref=dst,
            send_sem=self.send_sem.at[k],
            recv_sem=self.recv_sem.at[k],
            device_id=device,
            device_id_type=MESH,
        )
        copy.start()
        self.all.append(copy)
        return copy

    def finish(self):
        for copy in self.all:
            copy.wait_send()


def span(start, size, step):
    return pl.ds(pl.multiple_of(start, step), size)


class Reduce:
    def __init__(self, ring, copies, index, order, g_ref, out_ref, bufs):
        self.ring, self.copies = ring, copies
        self.order = order
        self.g, self.out = g_ref, out_ref
        self.core_buf, self.acc1, self.buf1, self.acc2, self.buf2, self.acc3, self.buf3, self.buf4 = bufs
        self.width = g_ref.shape[1]
        rows = self.width
        self.rows = rows
        self.n1 = rows // 2
        self.n2 = self.n1 // 4
        self.n3 = self.n2 // 4
        self.base = index * rows
        self.b1, self.b2, self.b3 = index * self.n1, index * self.n2, index * self.n3
        self.cols = self.width // NEAR

    def wait(self):
        for copy in self.flight:
            copy.wait_recv()

    def mine(self, level, a1=None, a2=None):
        r = self.ring
        at = self.base + r.core * self.n1
        if level >= 1:
            at = at + (getattr(r, self.order[0]) if a1 is None else a1) * self.n2
        if level >= 2:
            at = at + (getattr(r, self.order[1]) if a2 is None else a2) * self.n3
        return span(at, (self.n1, self.n2, self.n3)[level], 16)

    def s0(self):
        r = self.ring
        _, _, peers = r.peers("core")
        ((_, other, device),) = peers
        src = self.g.at[span(self.base + other * self.n1, self.n1, 16)]
        self.flight = [self.copies.start(src, self.core_buf.at[pl.ds(self.b1, self.n1)], device)]

    def s1(self):
        self.wait()
        mine = self.g[self.mine(0), :].astype(F32)
        here = pl.ds(self.b1, self.n1)
        self.acc1[here] = (mine + self.core_buf[here].astype(F32)).astype(BF16)
        _, _, peers = self.ring.peers(self.order[0])
        self.flight = []
        for d, to, device in peers:
            src = self.acc1.at[span(self.b1 + to * self.n2, self.n2, 16)]
            dst = self.buf1.at[d - 1, pl.ds(self.b2, self.n2)]
            self.flight.append(self.copies.start(src, dst, device))

    def s2(self):
        self.wait()
        me, n, _ = self.ring.peers(self.order[0])
        total = self.acc1[span(self.b1 + me * self.n2, self.n2, 16), :].astype(F32)
        here = pl.ds(self.b2, self.n2)
        for d in range(n - 1):
            total = total + self.buf1[d, here].astype(F32)
        self.acc2[here] = total.astype(BF16)
        _, _, peers = self.ring.peers(self.order[1])
        self.flight = []
        for d, to, device in peers:
            src = self.acc2.at[span(self.b2 + to * self.n3, self.n3, 16)]
            dst = self.buf2.at[d - 1, pl.ds(self.b3, self.n3)]
            self.flight.append(self.copies.start(src, dst, device))

    def s3(self):
        self.wait()
        me, n, _ = self.ring.peers(self.order[1])
        total = self.acc2[span(self.b2 + me * self.n3, self.n3, 16), :].astype(F32)
        here = pl.ds(self.b3, self.n3)
        for d in range(n - 1):
            total = total + self.buf2[d, here].astype(F32)
        self.acc3[here] = total.astype(BF16)
        _, _, peers = self.ring.peers("near")
        self.flight = []
        for d, to, device in peers:
            src = self.acc3.at[here, span(to * self.cols, self.cols, 128)]
            dst = self.buf3.at[d - 1, here]
            self.flight.append(self.copies.start(src, dst, device))

    def s4(self):
        self.wait()
        me, n, _ = self.ring.peers("near")
        here = pl.ds(self.b3, self.n3)
        total = self.acc3[here, span(me * self.cols, self.cols, 128)].astype(F32)
        for d in range(n - 1):
            total = total + self.buf3[d, here].astype(F32)
        far, _, peers = self.ring.peers("far")
        self.buf4[far, here] = total.astype(BF16)
        self.flight = []
        for _, _, device in peers:
            slot = self.buf4.at[far, here]
            self.flight.append(self.copies.start(slot, slot, device))

    def s5(self):
        self.wait()
        here = pl.ds(self.b3, self.n3)
        _, n, _ = self.ring.peers("far")
        total = self.buf4[0, here].astype(F32)
        for k in range(1, n):
            total = total + self.buf4[k, here].astype(F32)
        me, _, peers = self.ring.peers("near")
        rows, cols = self.mine(2), span(me * self.cols, self.cols, 128)
        self.out[rows, cols] = total.astype(BF16)
        self.flight = []
        for _, _, device in peers:
            part = self.out.at[rows, cols]
            self.flight.append(self.copies.start(part, part, device))

    def spread(self, axis, level):
        self.wait()
        _, _, peers = self.ring.peers(axis)
        part = self.out.at[self.mine(level)]
        self.flight = [self.copies.start(part, part, device) for _, _, device in peers]

    def s6(self):
        self.spread(self.order[1], 2)

    def s7(self):
        self.spread(self.order[0], 1)

    def s8(self):
        self.spread("core", 0)

    def s9(self):
        self.wait()


class Vector:
    AXES = ("core", "y", "x", "near", "far")

    def __init__(self, ring, copies, buf):
        self.ring, self.copies, self.buf = ring, copies, buf
        self.step = 0

    def start(self, value):
        me, n, peers = self.ring.peers(self.AXES[self.step])
        self.buf[self.step, me] = value
        slot = self.buf.at[self.step, me]
        self.flight = [self.copies.start(slot, slot, device) for _, _, device in peers]
        self.n = n

    def total(self):
        for copy in self.flight:
            copy.wait_recv()
        total = self.buf[self.step, 0]
        for k in range(1, self.n):
            total = total + self.buf[self.step, k]
        self.step += 1
        return total

    def next(self):
        self.start(self.total())


def greet(ring):
    barrier = pltpu.get_barrier_semaphore()
    count = 0
    for axis in ("far", "near", "y", "x", "core"):
        for _, _, device in ring.peers(axis)[2]:
            pl.semaphore_signal(barrier, inc=1, device_id=device, device_id_type=MESH)
            count += 1
    outer = ring.beside(2 * ring.core - 1)
    pl.semaphore_signal(barrier, inc=1, device_id=outer, device_id_type=MESH)
    return barrier, count + 1


def prep_kernel(
    grid_hbm,
    cot_hbm,
    own_hbm,
    w_send_hbm,
    w_recv_hbm,
    w_out_hbm,
    bias_hbm,
    gain_hbm,
    sender_hbm,
    recv_hbm,
    live_hbm,
    table,
    pick,
    pick_t,
    win,
    grid,
    cot,
    w_send,
    w_recv,
    w_out,
    bias,
    gain,
    index,
    mesh_buf,
    local_sem,
    send_sem,
    recv_sem,
):
    ring = Ring()
    barrier = pltpu.get_barrier_semaphore()
    for step in (-1, 1):
        pl.semaphore_signal(barrier, inc=1, device_id=ring.beside(step), device_id_type=MESH)
    loads = []
    for src, dst in (
        (own_hbm, mesh_buf.at[1]),
        (sender_hbm, index.at[0]),
        (recv_hbm, index.at[1]),
        (live_hbm, index.at[2]),
        (grid_hbm, grid),
        (w_recv_hbm, w_recv),
        (w_send_hbm, w_send),
        (w_out_hbm, w_out),
        (cot_hbm, cot),
        (bias_hbm, bias),
        (gain_hbm, gain),
    ):
        copy = pltpu.make_async_copy(src, dst, local_sem.at[len(loads)])
        copy.start()
        loads.append(copy)
    grid_rows, width = grid.shape
    slots = index.shape[2]
    mesh_rows = mesh_buf.shape[1]
    for copy in loads[:4]:
        copy.wait()
    pl.semaphore_wait(barrier, 2)
    copies = Copies(send_sem, recv_sem)
    halo = [
        copies.start(mesh_buf.at[1], mesh_buf.at[0], ring.beside(1)),
        copies.start(mesh_buf.at[1], mesh_buf.at[2], ring.beside(-1)),
    ]

    def build(i, carry):
        at = pl.multiple_of(i * 128, 128)
        sender = index[0, :, pl.ds(at, 128)]
        target = ring.space + (sender >> 3) - 1
        inside = (target >= 0) & (target < ring.count)
        row = jnp.where(inside, sender, mesh_rows + (sender & (mesh_rows - 1)))
        recv = jnp.where(index[2, :, pl.ds(at, 128)] > 0, index[1, :, pl.ds(at, 128)], -1)
        recv_b = jnp.broadcast_to(recv, (128, 128))
        row_b = jnp.broadcast_to(row, (128, 128))
        recv_c = recv_b.T
        row_c = row_b.T
        lane = lax.broadcasted_iota(jnp.int32, (128, 128), 1)
        sub = lax.broadcasted_iota(jnp.int32, (128, 128), 0)
        for k in range(grid_rows // 128):
            pick[pl.ds(at, 128), k * 128 : (k + 1) * 128] = (lane + k * 128 == recv_c).astype(
                F32
            ).astype(BF16)
            pick_t[k * 128 : (k + 1) * 128, pl.ds(at, 128)] = (sub + k * 128 == recv_b).astype(
                F32
            ).astype(BF16)
        pick[pl.ds(at, 128), grid_rows : grid_rows + PAD] = (lane == row_c).astype(F32).astype(BF16)
        pick_t[grid_rows : grid_rows + PAD, pl.ds(at, 128)] = (
            (sub == row_b).astype(F32).astype(BF16)
        )
        return carry

    lax.fori_loop(0, slots // 128, build, 0)
    loads[4].wait()
    loads[5].wait()
    table[0:grid_rows] = mm(grid[...], w_recv[...]).astype(BF16)
    table[grid_rows : grid_rows + PAD] = jnp.zeros((PAD, width), BF16)
    loads[6].wait()
    for copy in halo:
        copy.wait_recv()
    for k in range(3):
        win[k * mesh_rows : (k + 1) * mesh_rows] = mesh_buf[k]
    win[3 * mesh_rows : 4 * mesh_rows] = jnp.zeros((mesh_rows, width), BF16)
    window = win.shape[0]
    table[grid_rows : grid_rows + window] = mm(win[...], w_send[...]).astype(BF16)
    for copy in loads[7:]:
        copy.wait()
    copies.finish()


def prep_call(grid, cot, own, w_send, w_recv, w_out, bias, gain, sender, recv, live):
    grid_rows, width = grid.shape
    slots = recv.shape[1]
    mesh_rows = own.shape[0]
    vmem = pl.BlockSpec(memory_space=pltpu.VMEM)
    anywhere = pl.BlockSpec(memory_space=pltpu.HBM)
    square = jax.ShapeDtypeStruct((width, width), BF16)
    outs = (
        jax.ShapeDtypeStruct((grid_rows + PAD, width), BF16),
        jax.ShapeDtypeStruct((slots, grid_rows + PAD), BF16),
        jax.ShapeDtypeStruct((grid_rows + PAD, slots), BF16),
        jax.ShapeDtypeStruct((4 * mesh_rows, width), BF16),
        jax.ShapeDtypeStruct(grid.shape, BF16),
        jax.ShapeDtypeStruct(cot.shape, BF16),
        square,
        square,
        square,
        jax.ShapeDtypeStruct(bias.shape, F32),
        jax.ShapeDtypeStruct(gain.shape, F32),
    )
    return pl.pallas_call(
        prep_kernel,
        out_shape=outs,
        in_specs=[anywhere] * 11,
        out_specs=(vmem,) * len(outs),
        scratch_shapes=[
            pltpu.VMEM((3, 1, slots), jnp.int32),
            pltpu.VMEM((3, mesh_rows, width), BF16),
            pltpu.SemaphoreType.DMA((11,)),
            pltpu.SemaphoreType.DMA((2,)),
            pltpu.SemaphoreType.DMA((2,)),
        ],
        compiler_params=pltpu.CompilerParams(
            vmem_limit_bytes=PREP_VMEM, collective_id=0, has_side_effects=True
        ),
    )(*(pltpu.with_memory_space_constraint(a, pltpu.HBM) for a in (grid, cot, own, w_send, w_recv, w_out, bias, gain, sender, recv, live)))


def comm_scratch(width, grid_rows, mesh_rows, nx, ny):
    rows = 3 * width
    n1 = rows // 2
    n2 = n1 // 4
    n3 = n2 // 4
    cols = width // NEAR
    far = DEPTH // NEAR
    copies = 160
    return [
        pltpu.VMEM((rows, width), BF16),
        pltpu.VMEM((n1, width), BF16),
        pltpu.VMEM((n1, width), BF16),
        pltpu.VMEM((3, n2, width), BF16),
        pltpu.VMEM((n2, width), BF16),
        pltpu.VMEM((3, n3, width), BF16),
        pltpu.VMEM((n3, width), BF16),
        pltpu.VMEM((NEAR - 1, n3, cols), BF16),
        pltpu.VMEM((far, n3, cols), BF16),
        pltpu.VMEM((5, 4, 2, width), F32),
        pltpu.VMEM((nx - 1, grid_rows // nx, width), BF16),
        pltpu.VMEM((2, mesh_rows, width), F32),
        pltpu.SemaphoreType.DMA((copies,)),
        pltpu.SemaphoreType.DMA((copies,)),
    ]


def main_kernel(
    table,
    pick,
    pick_t,
    win_ref,
    grid_ref,
    cot_ref,
    w_send_ref,
    w_recv_ref,
    w_out_ref,
    bias_ref,
    gain_ref,
    out,
    vec_out_ref,
    d_grid_ref,
    d_mesh_ref,
    total,
    g_ref,
    level_ref,
    grads_ref,
    hid,
    dact,
    douter,
    dpre,
    *comm,
):
    *bufs, vec_buf, level_buf, halo_buf, send_sem, recv_sem = comm
    ring = Ring()
    barrier, count = greet(ring)
    grid_rows, width = grid_ref.shape
    slots = pick.shape[0]
    window = win_ref.shape[0]
    mesh_rows = halo_buf.shape[1]
    bias = bias_ref[...]
    gain = gain_ref[...]
    scale = 1.0 / width

    def forward(i, acc):
        at = pl.multiple_of(i * BLOCK, BLOCK)
        rows = pl.ds(at, BLOCK)
        preact = mm(pick[rows, :], table[...]) + bias
        half = 0.5 * preact
        turn = jnp.tanh(half)
        hidden = half + half * turn
        sig = 0.5 + 0.5 * turn
        hidden_b = hidden.astype(BF16)
        hid[rows, :] = hidden_b
        dact[rows, :] = sig + (hidden - hidden * sig)
        outer = mm(hidden_b, w_out_ref[...])
        upstream = mm(pick[rows, 0:grid_rows], cot_ref[...])
        center = outer - jnp.sum(outer, axis=-1, keepdims=True) * scale
        inv = lax.rsqrt(jnp.sum(center * center, axis=-1, keepdims=True) * scale + 1e-05)
        normed = center * inv
        scaled = upstream * gain
        m1 = jnp.sum(scaled, axis=-1, keepdims=True) * scale
        m2 = jnp.sum(scaled * normed, axis=-1, keepdims=True) * scale
        douter[rows, :] = (inv * (scaled - m1 - normed * m2)).astype(BF16)
        part = upstream * normed
        return acc + jnp.sum(part.reshape(BLOCK // 8, 8, width), axis=0)

    gain_acc = lax.fori_loop(0, slots // BLOCK, forward, jnp.zeros((8, width), F32))
    g_ref[2 * width : 3 * width] = mm(hid[...], douter[...], TN).astype(BF16)
    pl.semaphore_wait(barrier, count)
    copies = Copies(send_sem, recv_sem)
    early = [Reduce(ring, copies, i, order, g_ref, total, bufs) for i, order in EARLY]
    late = [Reduce(ring, copies, i, order, g_ref, total, bufs) for i, order in LATE]
    parts = early + late
    for part in early:
        part.s0()

    def backward(i, acc):
        at = pl.multiple_of(i * BLOCK, BLOCK)
        rows = pl.ds(at, BLOCK)
        d_pre = mm(douter[rows, :], w_out_ref[...], NT) * dact[rows, :]
        dpre[rows, :] = d_pre.astype(BF16)
        return acc + jnp.sum(d_pre.reshape(BLOCK // 8, 8, width), axis=0)

    bias_acc = lax.fori_loop(0, slots // BLOCK, backward, jnp.zeros((8, width), F32))
    for part in early:
        part.s1()
    sums = mm(pick_t[...], dpre[...])
    level = sums[0:grid_rows].astype(BF16)
    level_ref[...] = level
    grads = sums[grid_rows : grid_rows + window]
    grads_ref[...] = grads
    g_ref[width : 2 * width] = mm(grid_ref[...], level, TN).astype(BF16)
    g_ref[0:width] = mm(win_ref[...], grads.astype(BF16), TN).astype(BF16)
    for part in late:
        part.s0()
    vec = Vector(ring, copies, vec_buf)
    pair = jnp.concatenate(
        [jnp.sum(bias_acc, axis=0, keepdims=True), jnp.sum(gain_acc, axis=0, keepdims=True)], axis=0
    )
    vec.start(pair)
    for part in late:
        part.s1()
    vec.next()
    halo = [
        copies.start(grads_ref.at[pl.ds(2 * mesh_rows, mesh_rows)], halo_buf.at[0], ring.beside(1)),
        copies.start(grads_ref.at[pl.ds(0, mesh_rows)], halo_buf.at[1], ring.beside(-1)),
    ]
    for part in parts:
        part.s2()
    vec.next()
    share = level_buf.shape[1]
    x, _, x_peers = ring.peers("x")
    levels = []
    for d, to, device in x_peers:
        src = level_ref.at[span(to * share, share, 16)]
        levels.append(copies.start(src, level_buf.at[d - 1], device))
    for part in parts:
        part.s3()
    vec.next()
    for part in parts:
        part.s4()
    vec.next()
    for copy in halo:
        copy.wait_recv()
    mesh_sum = grads_ref[mesh_rows : 2 * mesh_rows] + halo_buf[0] + halo_buf[1]
    d_mesh_ref[...] = mm(mesh_sum.astype(BF16), w_send_ref[...], NT)
    for copy in levels:
        copy.wait_recv()
    grid_sum = level_ref[span(x * share, share, 16), :].astype(F32)
    for d in range(len(levels)):
        grid_sum = grid_sum + level_buf[d].astype(F32)
    d_grid_ref[...] = mm(grid_sum.astype(BF16), w_recv_ref[...], NT)
    for part in parts:
        part.s5()
    vec_out_ref[...] = vec.total()
    for part in parts:
        part.s6()
    for part in parts:
        part.s7()
    for part in parts:
        part.s8()
    for part in parts:
        part.s9()
    out[...] = total[...]
    copies.finish()


def main_call(inputs, mesh_rows):
    grid_rows, width = inputs[4].shape
    slots = inputs[1].shape[0]
    nx = lax.axis_size("level")
    ny = lax.axis_size("space") // (2 * DEPTH)
    vmem = pl.BlockSpec(memory_space=pltpu.VMEM)
    comm = comm_scratch(width, grid_rows, mesh_rows, nx, ny)
    return pl.pallas_call(
        main_kernel,
        out_shape=(
            jax.ShapeDtypeStruct((3 * width, width), BF16),
            jax.ShapeDtypeStruct((2, width), F32),
            jax.ShapeDtypeStruct((grid_rows // nx, width), F32),
            jax.ShapeDtypeStruct((mesh_rows, width), F32),
        ),
        in_specs=[vmem] * len(inputs),
        out_specs=(vmem,) * 4,
        scratch_shapes=[
            comm[0],
            pltpu.VMEM((3 * width, width), BF16),
            pltpu.VMEM((grid_rows, width), BF16),
            pltpu.VMEM((4 * mesh_rows, width), F32),
            pltpu.VMEM((slots, width), BF16),
            pltpu.VMEM((slots, width), F32),
            pltpu.VMEM((slots, width), BF16),
            pltpu.VMEM((slots, width), BF16),
            *comm[1:],
        ],
        compiler_params=pltpu.CompilerParams(
            vmem_limit_bytes=MAIN_VMEM, collective_id=1, has_side_effects=True
        ),
    )(*inputs)


def tail_kernel(total, vec, d_grid, d_mesh, *refs):
    *outs, sem = refs
    width = total.shape[1]
    sources = [
        d_grid,
        d_mesh,
        *(total.at[pl.ds(k * width, width)] for k in range(3)),
        vec.at[pl.ds(0, 1)],
        vec.at[pl.ds(1, 1)],
    ]
    copies = [
        pltpu.make_async_copy(src, dst, sem.at[k]) for k, (src, dst) in enumerate(zip(sources, outs))
    ]
    for copy in copies:
        copy.start()
    for copy in copies:
        copy.wait()


def tail_call(total, vec, d_grid, d_mesh):
    width = total.shape[1]
    vmem = pl.BlockSpec(memory_space=pltpu.VMEM)
    anywhere = pl.BlockSpec(memory_space=pl.ANY)
    square = jax.ShapeDtypeStruct((width, width), BF16)
    line = jax.ShapeDtypeStruct((1, width), F32)
    outs = (
        jax.ShapeDtypeStruct(d_grid.shape, F32),
        jax.ShapeDtypeStruct(d_mesh.shape, F32),
        square,
        square,
        square,
        line,
        line,
    )
    return pl.pallas_call(
        tail_kernel,
        out_shape=outs,
        in_specs=[vmem] * 4,
        out_specs=(anywhere,) * len(outs),
        scratch_shapes=[pltpu.SemaphoreType.DMA((len(outs),))],
        compiler_params=pltpu.CompilerParams(vmem_limit_bytes=1 << 20),
    )(total, vec, d_grid, d_mesh)


def body(
    grid_latent,
    mesh_latent,
    grid_output_cotangent,
    w_send,
    w_recv,
    output_weight,
    hidden_layer_bias,
    output_norm_gain,
    edge_sender,
    edge_receiver,
    edge_live,
):
    inputs = prep_call(
        grid_latent,
        grid_output_cotangent,
        mesh_latent[0],
        w_send,
        w_recv,
        output_weight,
        hidden_layer_bias[None],
        output_norm_gain[None],
        edge_sender,
        edge_receiver,
        edge_live,
    )
    results = main_call(inputs, mesh_latent.shape[1])
    d_grid, d_mesh, d_w_send, d_w_recv, d_w_out, d_bias, d_gain = tail_call(*results)
    return (d_grid, d_mesh[None], d_w_send, d_w_recv, d_w_out, d_bias[0], d_gain[0])


def solution(mesh):
    return jax.shard_map(
        body,
        mesh=mesh,
        in_specs=(
            P("space", None),
            P("level", "space", None),
            P("space", None),
            P(),
            P(),
            P(),
            P(),
            P(),
            P("level", "space"),
            P("level", "space"),
            P("level", "space"),
        ),
        out_specs=(P(("space", "level"), None), P("level", "space", None), P(), P(), P(), P(), P()),
        check_vma=False,
    )
```

```python
import jax
import jax.numpy as jnp
from jax import lax
from jax.experimental import pallas as pl
from jax.experimental.pallas import tpu as pltpu
from jax.sharding import PartitionSpec as P

F32 = jnp.float32
BF16 = jnp.bfloat16
NT = (((1,), (1,)), ((), ()))
TN = (((0,), (0,)), ((), ()))
PAD = 128
BLOCK = 256
STRIP = 16
PREP_VMEM = 24 << 20
MAIN_VMEM = 40 << 20


def mm(a, b, dims=(((1,), (0,)), ((), ()))):
    return lax.dot_general(a, b, dims, preferred_element_type=F32)


MESH = pl.DeviceIdType.MESH
DEPTH = 16
NEAR = 4
EARLY = ((2, "yx"),)
LATE = ((1, "xy"), (0, "yx"))


class Ring:
    def __init__(self):
        space = lax.axis_index("space")
        self.count = lax.axis_size("space")
        self.x = lax.axis_index("level")
        self.nx = lax.axis_size("level")
        self.ny = self.count // (2 * DEPTH)
        self.space = space
        self.core = lax.rem(space, 2)
        z = lax.rem(space // 2, DEPTH)
        self.y = space // (2 * DEPTH)
        self.near = lax.rem(z, NEAR)
        self.far = z // NEAR

    def at(self, core=None, y=None, near=None, far=None, x=None):
        core = self.core if core is None else core
        y = self.y if y is None else y
        near = self.near if near is None else near
        far = self.far if far is None else far
        x = self.x if x is None else x
        return {"space": ((y * DEPTH) + far * NEAR + near) * 2 + core, "level": x}

    def peers(self, axis):
        me, n = {
            "core": (self.core, 2),
            "y": (self.y, self.ny),
            "x": (self.x, self.nx),
            "near": (self.near, NEAR),
            "far": (self.far, DEPTH // NEAR),
        }[axis]
        out = []
        for d in range(1, n):
            to = lax.rem(me + d, n)
            out.append((d, to, self.at(**{axis: to})))
        return me, n, out

    def beside(self, step):
        return {"space": lax.rem(self.space + step + self.count, self.count), "level": self.x}


class Copies:
    def __init__(self, send_sem, recv_sem):
        self.send_sem, self.recv_sem = send_sem, recv_sem
        self.used = 0
        self.all = []

    def start(self, src, dst, device):
        k = self.used
        self.used += 1
        copy = pltpu.make_async_remote_copy(
            src_ref=src,
            dst_ref=dst,
            send_sem=self.send_sem.at[k],
            recv_sem=self.recv_sem.at[k],
            device_id=device,
            device_id_type=MESH,
        )
        copy.start()
        self.all.append(copy)
        return copy

    def finish(self):
        for copy in self.all:
            copy.wait_send()


def span(start, size, step):
    return pl.ds(pl.multiple_of(start, step), size)


class Reduce:
    def __init__(self, ring, copies, index, order, g_ref, out_ref, bufs):
        self.ring, self.copies = ring, copies
        self.order = order
        self.g, self.out = g_ref, out_ref
        self.core_buf, self.acc1, self.buf1, self.acc2, self.buf2, self.acc3, self.buf3, self.buf4 = bufs
        self.width = g_ref.shape[1]
        rows = self.width
        self.rows = rows
        self.n1 = rows // 2
        self.n2 = self.n1 // 4
        self.n3 = self.n2 // 4
        self.base = index * rows
        self.b1, self.b2, self.b3 = index * self.n1, index * self.n2, index * self.n3
        self.cols = self.width // NEAR

    def wait(self):
        for copy in self.flight:
            copy.wait_recv()

    def mine(self, level, a1=None, a2=None):
        r = self.ring
        at = self.base + r.core * self.n1
        if level >= 1:
            at = at + (getattr(r, self.order[0]) if a1 is None else a1) * self.n2
        if level >= 2:
            at = at + (getattr(r, self.order[1]) if a2 is None else a2) * self.n3
        return span(at, (self.n1, self.n2, self.n3)[level], 16)

    def s0(self):
        r = self.ring
        _, _, peers = r.peers("core")
        ((_, other, device),) = peers
        src = self.g.at[span(self.base + other * self.n1, self.n1, 16)]
        self.flight = [self.copies.start(src, self.core_buf.at[pl.ds(self.b1, self.n1)], device)]

    def s1(self):
        self.wait()
        mine = self.g[self.mine(0), :].astype(F32)
        here = pl.ds(self.b1, self.n1)
        self.acc1[here] = (mine + self.core_buf[here].astype(F32)).astype(BF16)
        _, _, peers = self.ring.peers(self.order[0])
        self.flight = []
        for d, to, device in peers:
            src = self.acc1.at[span(self.b1 + to * self.n2, self.n2, 16)]
            dst = self.buf1.at[d - 1, pl.ds(self.b2, self.n2)]
            self.flight.append(self.copies.start(src, dst, device))

    def s2(self):
        self.wait()
        me, n, _ = self.ring.peers(self.order[0])
        total = self.acc1[span(self.b1 + me * self.n2, self.n2, 16), :].astype(F32)
        here = pl.ds(self.b2, self.n2)
        for d in range(n - 1):
            total = total + self.buf1[d, here].astype(F32)
        self.acc2[here] = total.astype(BF16)
        _, _, peers = self.ring.peers(self.order[1])
        self.flight = []
        for d, to, device in peers:
            src = self.acc2.at[span(self.b2 + to * self.n3, self.n3, 16)]
            dst = self.buf2.at[d - 1, pl.ds(self.b3, self.n3)]
            self.flight.append(self.copies.start(src, dst, device))

    def s3(self):
        self.wait()
        me, n, _ = self.ring.peers(self.order[1])
        total = self.acc2[span(self.b2 + me * self.n3, self.n3, 16), :].astype(F32)
        here = pl.ds(self.b3, self.n3)
        for d in range(n - 1):
            total = total + self.buf2[d, here].astype(F32)
        self.acc3[here] = total.astype(BF16)
        _, _, peers = self.ring.peers("near")
        self.flight = []
        for d, to, device in peers:
            src = self.acc3.at[here, span(to * self.cols, self.cols, 128)]
            dst = self.buf3.at[d - 1, here]
            self.flight.append(self.copies.start(src, dst, device))

    def s4(self):
        self.wait()
        me, n, _ = self.ring.peers("near")
        here = pl.ds(self.b3, self.n3)
        total = self.acc3[here, span(me * self.cols, self.cols, 128)].astype(F32)
        for d in range(n - 1):
            total = total + self.buf3[d, here].astype(F32)
        far, _, peers = self.ring.peers("far")
        self.buf4[far, here] = total.astype(BF16)
        self.flight = []
        for _, _, device in peers:
            slot = self.buf4.at[far, here]
            self.flight.append(self.copies.start(slot, slot, device))

    def s5(self):
        self.wait()
        here = pl.ds(self.b3, self.n3)
        _, n, _ = self.ring.peers("far")
        total = self.buf4[0, here].astype(F32)
        for k in range(1, n):
            total = total + self.buf4[k, here].astype(F32)
        me, _, peers = self.ring.peers("near")
        rows, cols = self.mine(2), span(me * self.cols, self.cols, 128)
        self.out[rows, cols] = total.astype(BF16)
        self.flight = []
        for _, _, device in peers:
            part = self.out.at[rows, cols]
            self.flight.append(self.copies.start(part, part, device))

    def spread(self, axis, level):
        self.wait()
        _, _, peers = self.ring.peers(axis)
        part = self.out.at[self.mine(level)]
        self.flight = [self.copies.start(part, part, device) for _, _, device in peers]

    def s6(self):
        self.spread(self.order[1], 2)

    def s7(self):
        self.spread(self.order[0], 1)

    def s8(self):
        self.spread("core", 0)

    def s9(self):
        self.wait()


class Vector:
    AXES = ("core", "y", "x", "near", "far")

    def __init__(self, ring, copies, buf):
        self.ring, self.copies, self.buf = ring, copies, buf
        self.step = 0

    def start(self, value):
        me, n, peers = self.ring.peers(self.AXES[self.step])
        self.buf[self.step, me] = value
        slot = self.buf.at[self.step, me]
        self.flight = [self.copies.start(slot, slot, device) for _, _, device in peers]
        self.n = n

    def total(self):
        for copy in self.flight:
            copy.wait_recv()
        total = self.buf[self.step, 0]
        for k in range(1, self.n):
            total = total + self.buf[self.step, k]
        self.step += 1
        return total

    def next(self):
        self.start(self.total())


def greet(ring):
    barrier = pltpu.get_barrier_semaphore()
    count = 0
    for axis in ("far", "near", "y", "x", "core"):
        for _, _, device in ring.peers(axis)[2]:
            pl.semaphore_signal(barrier, inc=1, device_id=device, device_id_type=MESH)
            count += 1
    outer = ring.beside(2 * ring.core - 1)
    pl.semaphore_signal(barrier, inc=1, device_id=outer, device_id_type=MESH)
    return barrier, count + 1


def prep_kernel(
    grid_hbm,
    cot_hbm,
    own_hbm,
    w_send_hbm,
    w_recv_hbm,
    w_out_hbm,
    bias_hbm,
    gain_hbm,
    sender_hbm,
    recv_hbm,
    live_hbm,
    table,
    pick,
    pick_t,
    win,
    grid,
    cot,
    w_send,
    w_recv,
    w_out,
    w_back,
    gain,
    bias,
    index,
    mesh_buf,
    local_sem,
    send_sem,
    recv_sem,
):
    ring = Ring()
    barrier = pltpu.get_barrier_semaphore()
    for step in (-1, 1):
        pl.semaphore_signal(barrier, inc=1, device_id=ring.beside(step), device_id_type=MESH)
    loads = []
    for src, dst in (
        (own_hbm, mesh_buf.at[1]),
        (sender_hbm, index.at[0]),
        (recv_hbm, index.at[1]),
        (live_hbm, index.at[2]),
        (grid_hbm, grid),
        (w_recv_hbm, w_recv),
        (w_send_hbm, w_send),
        (w_out_hbm, w_out),
        (cot_hbm, cot),
        (bias_hbm, bias),
        (gain_hbm, gain),
    ):
        copy = pltpu.make_async_copy(src, dst, local_sem.at[len(loads)])
        copy.start()
        loads.append(copy)
    grid_rows, width = grid.shape
    slots = index.shape[2]
    mesh_rows = mesh_buf.shape[1]
    for copy in loads[:4]:
        copy.wait()
    pl.semaphore_wait(barrier, 2)
    copies = Copies(send_sem, recv_sem)
    halo = [
        copies.start(mesh_buf.at[1], mesh_buf.at[0], ring.beside(1)),
        copies.start(mesh_buf.at[1], mesh_buf.at[2], ring.beside(-1)),
    ]

    def build(i, carry):
        at = pl.multiple_of(i * 128, 128)
        sender = index[0, :, pl.ds(at, 128)]
        target = ring.space + (sender >> 3) - 1
        inside = (target >= 0) & (target < ring.count)
        row = jnp.where(inside, sender, mesh_rows + (sender & (mesh_rows - 1)))
        recv = jnp.where(index[2, :, pl.ds(at, 128)] > 0, index[1, :, pl.ds(at, 128)], -1)
        recv_b = jnp.broadcast_to(recv, (128, 128))
        row_b = jnp.broadcast_to(row, (128, 128))
        recv_c = recv_b.T
        row_c = row_b.T
        lane = lax.broadcasted_iota(jnp.int32, (128, 128), 1)
        sub = lax.broadcasted_iota(jnp.int32, (128, 128), 0)
        for k in range(grid_rows // 128):
            pick[pl.ds(at, 128), k * 128 : (k + 1) * 128] = (lane + k * 128 == recv_c).astype(
                F32
            ).astype(BF16)
            pick_t[k * 128 : (k + 1) * 128, pl.ds(at, 128)] = (sub + k * 128 == recv_b).astype(
                F32
            ).astype(BF16)
        pick[pl.ds(at, 128), grid_rows : grid_rows + PAD] = (lane == row_c).astype(F32).astype(BF16)
        pick_t[grid_rows : grid_rows + PAD, pl.ds(at, 128)] = (
            (sub == row_b).astype(F32).astype(BF16)
        )
        return carry

    lax.fori_loop(0, slots // 128, build, 0)
    loads[4].wait()
    loads[5].wait()
    loads[9].wait()
    table[0:grid_rows] = (0.5 * (mm(grid[...], w_recv[...]) + bias[...])).astype(BF16)
    table[grid_rows : grid_rows + PAD] = jnp.zeros((PAD, width), BF16)
    loads[7].wait()
    w_back[...] = (0.5 * w_out[...].astype(F32)).T.astype(BF16)
    loads[6].wait()
    for copy in halo:
        copy.wait_recv()
    for k in range(3):
        win[k * mesh_rows : (k + 1) * mesh_rows] = mesh_buf[k]
    win[3 * mesh_rows : 4 * mesh_rows] = jnp.zeros((mesh_rows, width), BF16)
    window = win.shape[0]
    send = mm(win[...], w_send[...]).astype(BF16)
    table[grid_rows : grid_rows + window] = (0.5 * send.astype(F32)).astype(BF16)
    loads[8].wait()
    loads[10].wait()
    copies.finish()


def prep_call(grid, cot, own, w_send, w_recv, w_out, bias, gain, sender, recv, live):
    grid_rows, width = grid.shape
    slots = recv.shape[1]
    mesh_rows = own.shape[0]
    vmem = pl.BlockSpec(memory_space=pltpu.VMEM)
    anywhere = pl.BlockSpec(memory_space=pltpu.HBM)
    square = jax.ShapeDtypeStruct((width, width), BF16)
    outs = (
        jax.ShapeDtypeStruct((grid_rows + PAD, width), BF16),
        jax.ShapeDtypeStruct((slots, grid_rows + PAD), BF16),
        jax.ShapeDtypeStruct((grid_rows + PAD, slots), BF16),
        jax.ShapeDtypeStruct((4 * mesh_rows, width), BF16),
        jax.ShapeDtypeStruct(grid.shape, BF16),
        jax.ShapeDtypeStruct(cot.shape, BF16),
        square,
        square,
        square,
        square,
        jax.ShapeDtypeStruct(gain.shape, F32),
    )
    return pl.pallas_call(
        prep_kernel,
        out_shape=outs,
        in_specs=[anywhere] * 11,
        out_specs=(vmem,) * len(outs),
        scratch_shapes=[
            pltpu.VMEM(bias.shape, F32),
            pltpu.VMEM((3, 1, slots), jnp.int32),
            pltpu.VMEM((3, mesh_rows, width), BF16),
            pltpu.SemaphoreType.DMA((11,)),
            pltpu.SemaphoreType.DMA((2,)),
            pltpu.SemaphoreType.DMA((2,)),
        ],
        compiler_params=pltpu.CompilerParams(
            vmem_limit_bytes=PREP_VMEM, collective_id=0, has_side_effects=True
        ),
    )(*(pltpu.with_memory_space_constraint(a, pltpu.HBM) for a in (grid, cot, own, w_send, w_recv, w_out, bias, gain, sender, recv, live)))


def comm_scratch(width, grid_rows, mesh_rows, nx, ny):
    rows = 3 * width
    n1 = rows // 2
    n2 = n1 // 4
    n3 = n2 // 4
    cols = width // NEAR
    far = DEPTH // NEAR
    copies = 160
    return [
        pltpu.VMEM((rows, width), BF16),
        pltpu.VMEM((n1, width), BF16),
        pltpu.VMEM((n1, width), BF16),
        pltpu.VMEM((3, n2, width), BF16),
        pltpu.VMEM((n2, width), BF16),
        pltpu.VMEM((3, n3, width), BF16),
        pltpu.VMEM((n3, width), BF16),
        pltpu.VMEM((NEAR - 1, n3, cols), BF16),
        pltpu.VMEM((far, n3, cols), BF16),
        pltpu.VMEM((5, 4, 2, width), F32),
        pltpu.VMEM((nx - 1, grid_rows // nx, width), BF16),
        pltpu.VMEM((2, mesh_rows, width), F32),
        pltpu.SemaphoreType.DMA((copies,)),
        pltpu.SemaphoreType.DMA((copies,)),
    ]


def main_kernel(
    table,
    pick,
    pick_t,
    win_ref,
    grid_ref,
    cot_ref,
    w_send_ref,
    w_recv_ref,
    w_out_ref,
    w_back_ref,
    gain_ref,
    total,
    vec_out_ref,
    d_grid_ref,
    d_mesh_ref,
    g_ref,
    level_ref,
    grads_ref,
    hid,
    dact,
    douter,
    dpre,
    *rest,
):
    stage, comm = rest[:12], rest[12:]
    *bufs, vec_buf, level_buf, halo_buf, send_sem, recv_sem = comm
    ring = Ring()
    barrier, count = greet(ring)
    grid_rows, width = grid_ref.shape
    slots = pick.shape[0]
    window = win_ref.shape[0]
    mesh_rows = halo_buf.shape[1]
    gain = gain_ref[...]
    scale = 1.0 / width
    blocks = slots // BLOCK
    halves, hiddens, outers, ups, douters, backs = (stage[2 * k : 2 * k + 2] for k in range(6))

    def rows_at(i, r=0, size=BLOCK):
        start = i * BLOCK
        if not isinstance(i, int):
            start = pl.multiple_of(start, BLOCK)
        return pl.ds(start + r, size)

    def gather(i, slot):
        halves[slot][...] = mm(pick[rows_at(i), :], table[...])

    def activate(i, slot):
        for r in range(0, BLOCK, STRIP):
            strip = slice(r, r + STRIP)
            half = halves[slot][strip, :]
            turn = jnp.tanh(half)
            plus = 1.0 + turn
            hidden = half * plus
            hidden_b = hidden.astype(BF16)
            hiddens[slot][strip, :] = hidden_b
            hid[rows_at(i, r, STRIP), :] = hidden_b
            dact[rows_at(i, r, STRIP), :] = plus + hidden * (1.0 - turn)

    def project(i, slot):
        outers[slot][...] = mm(hiddens[slot][...], w_out_ref[...])
        ups[slot][...] = mm(pick[rows_at(i), 0:grid_rows], cot_ref[...])

    def normalize(i, slot, acc):
        for r in range(0, BLOCK, STRIP):
            strip = slice(r, r + STRIP)
            outer = outers[slot][strip, :]
            upstream = ups[slot][strip, :]
            center = outer - jnp.sum(outer, axis=-1, keepdims=True) * scale
            inv = lax.rsqrt(jnp.sum(center * center, axis=-1, keepdims=True) * scale + 1e-05)
            normed = center * inv
            scaled = upstream * gain
            part = upstream * normed
            m1 = jnp.sum(scaled, axis=-1, keepdims=True) * scale
            m2 = jnp.sum(part * gain, axis=-1, keepdims=True) * scale
            d_outer = (inv * (scaled - m1 - normed * m2)).astype(BF16)
            douters[slot][strip, :] = d_outer
            douter[rows_at(i, r, STRIP), :] = d_outer
            acc = acc + jnp.sum(part.reshape(STRIP // 8, 8, width), axis=0)
        return acc

    def back(i, slot):
        backs[slot][...] = mm(douters[slot][...], w_back_ref[...])

    def differentiate(i, slot, acc):
        for r in range(0, BLOCK, STRIP):
            d_pre = backs[slot][r : r + STRIP, :] * dact[rows_at(i, r, STRIP), :]
            dpre[rows_at(i, r, STRIP), :] = d_pre.astype(BF16)
            acc = acc + jnp.sum(d_pre.reshape(STRIP // 8, 8, width), axis=0)
        return acc

    def tick(t, parity, accs):
        bias_acc, gain_acc = accs

        def on(lag):
            return not isinstance(t, int) or 0 <= t - lag < blocks

        if on(5):
            bias_acc = differentiate(t - 5, (parity + 1) % 2, bias_acc)
        if on(4):
            back(t - 4, parity)
        if on(3):
            gain_acc = normalize(t - 3, (parity + 1) % 2, gain_acc)
        if on(2):
            project(t - 2, parity)
        if on(1):
            activate(t - 1, (parity + 1) % 2)
        if on(0):
            gather(t, parity)
        return bias_acc, gain_acc

    zero = jnp.zeros((8, width), F32)
    accs = (zero, zero)
    for t in range(6):
        accs = tick(t, t % 2, accs)

    def pair(j, accs):
        t = 6 + 2 * j
        return tick(t + 1, 1, tick(t, 0, accs))

    accs = lax.fori_loop(0, (blocks - 6) // 2, pair, accs)
    for t in range(blocks, blocks + 5):
        accs = tick(t, t % 2, accs)
    bias_acc, gain_acc = accs
    g_ref[2 * width : 3 * width] = mm(hid[...], douter[...], TN).astype(BF16)
    pl.semaphore_wait(barrier, count)
    copies = Copies(send_sem, recv_sem)
    early = [Reduce(ring, copies, i, order, g_ref, total, bufs) for i, order in EARLY]
    late = [Reduce(ring, copies, i, order, g_ref, total, bufs) for i, order in LATE]
    parts = early + late
    for part in early:
        part.s0()

    sums = mm(pick_t[...], dpre[...])
    for part in early:
        part.s1()
    level = sums[0:grid_rows].astype(BF16)
    level_ref[...] = level
    grads = sums[grid_rows : grid_rows + window]
    grads_ref[...] = grads
    g_ref[width : 2 * width] = mm(grid_ref[...], level, TN).astype(BF16)
    g_ref[0:width] = mm(win_ref[...], grads.astype(BF16), TN).astype(BF16)
    for part in late:
        part.s0()
    vec = Vector(ring, copies, vec_buf)
    pair = jnp.concatenate(
        [jnp.sum(bias_acc, axis=0, keepdims=True), jnp.sum(gain_acc, axis=0, keepdims=True)], axis=0
    )
    vec.start(pair)
    for part in late:
        part.s1()
    vec.next()
    halo = [
        copies.start(grads_ref.at[pl.ds(2 * mesh_rows, mesh_rows)], halo_buf.at[0], ring.beside(1)),
        copies.start(grads_ref.at[pl.ds(0, mesh_rows)], halo_buf.at[1], ring.beside(-1)),
    ]
    for part in parts:
        part.s2()
    vec.next()
    share = level_buf.shape[1]
    x, _, x_peers = ring.peers("x")
    levels = []
    for d, to, device in x_peers:
        src = level_ref.at[span(to * share, share, 16)]
        levels.append(copies.start(src, level_buf.at[d - 1], device))
    for part in parts:
        part.s3()
    vec.next()
    for part in parts:
        part.s4()
    vec.next()
    for copy in halo:
        copy.wait_recv()
    mesh_sum = grads_ref[mesh_rows : 2 * mesh_rows] + halo_buf[0] + halo_buf[1]
    d_mesh_ref[...] = mm(mesh_sum.astype(BF16), w_send_ref[...], NT)
    for part in parts:
        part.s5()
    vec_out_ref[...] = vec.total()
    for part in parts:
        part.s6()
    for copy in levels:
        copy.wait_recv()
    grid_sum = level_ref[span(x * share, share, 16), :].astype(F32)
    for d in range(len(levels)):
        grid_sum = grid_sum + level_buf[d].astype(F32)
    d_grid_ref[...] = mm(grid_sum.astype(BF16), w_recv_ref[...], NT)
    for part in parts:
        part.s7()
    for part in parts:
        part.s8()
    for part in parts:
        part.s9()
    copies.finish()


def main_call(inputs, mesh_rows):
    grid_rows, width = inputs[4].shape
    slots = inputs[1].shape[0]
    nx = lax.axis_size("level")
    ny = lax.axis_size("space") // (2 * DEPTH)
    vmem = pl.BlockSpec(memory_space=pltpu.VMEM)
    comm = comm_scratch(width, grid_rows, mesh_rows, nx, ny)
    return pl.pallas_call(
        main_kernel,
        out_shape=(
            jax.ShapeDtypeStruct((3 * width, width), BF16),
            jax.ShapeDtypeStruct((2, width), F32),
            jax.ShapeDtypeStruct((grid_rows // nx, width), F32),
            jax.ShapeDtypeStruct((mesh_rows, width), F32),
        ),
        in_specs=[vmem] * len(inputs),
        out_specs=(vmem,) * 4,
        scratch_shapes=[
            pltpu.VMEM((3 * width, width), BF16),
            pltpu.VMEM((grid_rows, width), BF16),
            pltpu.VMEM((4 * mesh_rows, width), F32),
            pltpu.VMEM((slots, width), BF16),
            pltpu.VMEM((slots, width), F32),
            pltpu.VMEM((slots, width), BF16),
            pltpu.VMEM((slots, width), BF16),
            *(pltpu.VMEM((BLOCK, width), BF16 if k in (1, 4) else F32) for k in range(6) for _ in range(2)),
            *comm[1:],
        ],
        compiler_params=pltpu.CompilerParams(
            vmem_limit_bytes=MAIN_VMEM, collective_id=1, has_side_effects=True
        ),
    )(*inputs)


def tail_kernel(total, vec, d_grid, d_mesh, *refs):
    *outs, sem = refs
    width = total.shape[1]
    sources = [
        d_grid,
        d_mesh,
        *(total.at[pl.ds(k * width, width)] for k in range(3)),
        vec.at[pl.ds(0, 1)],
        vec.at[pl.ds(1, 1)],
    ]
    copies = [
        pltpu.make_async_copy(src, dst, sem.at[k]) for k, (src, dst) in enumerate(zip(sources, outs))
    ]
    for copy in copies:
        copy.start()
    for copy in copies:
        copy.wait()


def tail_call(total, vec, d_grid, d_mesh):
    width = total.shape[1]
    vmem = pl.BlockSpec(memory_space=pltpu.VMEM)
    anywhere = pl.BlockSpec(memory_space=pl.ANY)
    square = jax.ShapeDtypeStruct((width, width), BF16)
    line = jax.ShapeDtypeStruct((1, width), F32)
    outs = (
        jax.ShapeDtypeStruct(d_grid.shape, F32),
        jax.ShapeDtypeStruct(d_mesh.shape, F32),
        square,
        square,
        square,
        line,
        line,
    )
    return pl.pallas_call(
        tail_kernel,
        out_shape=outs,
        in_specs=[vmem] * 4,
        out_specs=(anywhere,) * len(outs),
        scratch_shapes=[pltpu.SemaphoreType.DMA((len(outs),))],
        compiler_params=pltpu.CompilerParams(vmem_limit_bytes=1 << 20),
    )(total, vec, d_grid, d_mesh)


def body(
    grid_latent,
    mesh_latent,
    grid_output_cotangent,
    w_send,
    w_recv,
    output_weight,
    hidden_layer_bias,
    output_norm_gain,
    edge_sender,
    edge_receiver,
    edge_live,
):
    inputs = prep_call(
        grid_latent,
        grid_output_cotangent,
        mesh_latent[0],
        w_send,
        w_recv,
        output_weight,
        hidden_layer_bias[None],
        output_norm_gain[None],
        edge_sender,
        edge_receiver,
        edge_live,
    )
    results = main_call(inputs, mesh_latent.shape[1])
    d_grid, d_mesh, d_w_send, d_w_recv, d_w_out, d_bias, d_gain = tail_call(*results)
    return (d_grid, d_mesh[None], d_w_send, d_w_recv, d_w_out, d_bias[0], d_gain[0])


def solution(mesh):
    return jax.shard_map(
        body,
        mesh=mesh,
        in_specs=(
            P("space", None),
            P("level", "space", None),
            P("space", None),
            P(),
            P(),
            P(),
            P(),
            P(),
            P("level", "space"),
            P("level", "space"),
            P("level", "space"),
        ),
        out_specs=(P(("space", "level"), None), P("level", "space", None), P(), P(), P(), P(), P()),
        check_vma=False,
    )
```
